32 devices in a mesh: ga: 8 (over z, y), band: 4 (over x, core).
Axes of the slice: x: 2, y: 2, z: 4, core: 2. Of those that a mesh axis runs over, the one named last changes fastest.
Arguments:
- coeffs: bfloat16 [2048, 128], P('ga', 'band'), may hold values from -6 to 6
- coupling: bfloat16 [12288, 12288], P('ga', 'band'), may hold values from -0.21875 to 0.21875
- miller: int32 [3, 2048], P(None, 'ga'), may hold values from -24 to 24
- species: int32 [1024], replicated, may hold values from 0 to 3
- proj_atom: int32 [12288], replicated, may hold values from 0 to 1023, as said below
- positions: float32 [3, 1024], replicated, may hold values from 0 to 1
- radial: float32 [12, 128], replicated, may hold values from -8 to 8
Outputs:
- result: bfloat16 [2048, 128], P('ga', 'band')
The draws below stay inside these ranges and needn't reach their ends.
Inputs may be any that keep to these rules, and one draw needn't show every extreme that they name: `proj_atom`: projector p has channel p mod 12; each atom owns 12 consecutive projectors.
All inputs are finite; a program needn't handle non-finite values.
Results may differ from the reference program's by a relative error of at most 0.008.
Values may be sent and summed in bfloat16 or wider, within the bound.
No kernel may reach another device: no remote copies, remote signals or barrier semaphores. Data moves between devices by JAX's collectives and lax.ppermute only.
A program may use at most 128 MiB of HBM per device.

```python
import math
import jax
import jax.numpy as jnp
from jax import lax

ATOMS = 1024
NCH = 12
SHELLS = 3
KINDS = 4
QBINS = 128
MMAX = 24
PWD = 256
NPROJ = 12288
NPW = 2048
NBANDS = 128


def draw_proj_atom(key, part):
    order = jax.random.permutation(jax.random.fold_in(key, 17), ATOMS).astype(jnp.int32)
    return jnp.repeat(order, NCH).astype(jnp.int32)


def touch_ends(drawn, rng, low, high):
    shape = drawn.shape
    index_at = [jax.random.randint(jax.random.fold_in(rng, axis), (), 0, shape[axis]) for axis in range(len(shape))]
    drawn = drawn.at[tuple(index_at)].set(low)
    longest = shape.index(max(shape))
    index_at[longest] = (index_at[longest] + 1) % shape[longest]
    return drawn.at[tuple(index_at)].set(high)


def steps_of(stream_key, dims, pieces, low, high):
    gain = 1.0
    for axis_at, shards_of in pieces:
        steps = jax.random.uniform(jax.random.fold_in(jax.random.fold_in(stream_key, 6), axis_at), (shards_of,), jnp.float32, low / len(pieces), high / len(pieces))
        gain = gain * jnp.repeat(jnp.exp(steps), dims[axis_at] // shards_of).reshape((-1,) + (1,) * (len(dims) - 1 - axis_at))
    return gain


def centred(stream_key, extent, width, limit, split=(), held_as=jnp.bfloat16):
    factor_of = steps_of(stream_key, extent, split, -0.22, 0.18) if split else 1.0
    array = jax.random.normal(stream_key, extent, jnp.float32) * width * factor_of
    return jnp.minimum(jnp.maximum(array, -limit), limit).astype(held_as)


def setup_inputs(seed: int = 0) -> dict:
    splits = jax.random.split(jax.random.key(seed), 8)
    return {
        "coeffs": centred(splits[0], (NPW, NBANDS), 1.0, 6.0, ((0, 8), (1, 4))),
        "coupling": centred(splits[1], (NPROJ, NPROJ), (NPROJ // 16) ** -0.5, 0.21875, ((0, 8), (1, 4))),
        "miller": touch_ends(jax.random.randint(splits[2], (3, NPW), 0 - MMAX, MMAX + 1), jax.random.fold_in(splits[2], 1), 0 - MMAX, MMAX).astype(jnp.int32),
        "species": touch_ends(jax.random.randint(splits[3], (ATOMS,), 0, KINDS), jax.random.fold_in(splits[3], 1), 0, KINDS - 1).astype(jnp.int32),
        "proj_atom": draw_proj_atom(jax.random.fold_in(splits[7], 71), 0),
        "positions": jnp.clip(jax.random.uniform(splits[5], (3, ATOMS), jnp.float32, 0.0, 1.0), 0.0, 1.0),
        "radial": centred(splits[6], (KINDS * SHELLS, QBINS), 1.5, 8.0, (), jnp.float32),
    }


def radial_values(miller_block, radial):
    mf = miller_block.astype(jnp.float32)
    qval = (mf[0] * mf[0] + mf[1] * mf[1] + mf[2] * mf[2]) * ((QBINS - 1) / (3.0 * MMAX * MMAX))
    knots = jnp.arange(QBINS, dtype=jnp.int32).astype(jnp.float32)
    hats = jnp.maximum(0.0, 1.0 - jnp.abs(qval[:, None] - knots[None, :]))
    return jnp.dot(hats, radial.T, precision=lax.Precision.HIGHEST)

def make_beta(miller_block, radval, species, proj_atom, positions, start, count, scale):
    mf = miller_block.astype(jnp.float32)
    atoms = lax.dynamic_slice_in_dim(proj_atom, jnp.asarray(start).astype(jnp.int32), count)
    channel = (jnp.asarray(start).astype(jnp.int32) + jnp.arange(count, dtype=jnp.int32)) % NCH
    shell = channel // 4
    comp = channel % 4
    kind = jnp.take(species, atoms)
    column = kind * SHELLS + shell
    select = (column[None, :] == jnp.arange(KINDS * SHELLS, dtype=jnp.int32)[:, None]).astype(jnp.float32)
    radpart = jnp.dot(radval, select, precision=lax.Precision.HIGHEST)
    place = jnp.take(positions, atoms, axis=1)
    theta = 2.0 * math.pi * (mf[0][:, None] * place[0][None, :] + mf[1][:, None] * place[1][None, :] + mf[2][:, None] * place[2][None, :])
    unit = mf / MMAX
    angular = jnp.where(comp[None, :] == 1, unit[0][:, None], jnp.where(comp[None, :] == 2, unit[1][:, None], jnp.where(comp[None, :] == 3, unit[2][:, None], jnp.ones_like(theta))))
    phase = jnp.where(comp[None, :] == 0, jnp.cos(theta), jnp.sin(theta))
    return (radpart * angular * phase * scale).astype(jnp.bfloat16)

def reference(coeffs, coupling, miller, species, proj_atom, positions, radial):
    scale = 1.0 / math.sqrt(NPW)
    blocks = NPW // PWD
    miller_blocks = miller.reshape(3, blocks, PWD).transpose(1, 0, 2)
    coeff_blocks = coeffs.reshape(blocks, PWD, NBANDS)

    def project(total, item):
        mblock, cblock = item
        radval = radial_values(mblock, radial)
        beta = make_beta(mblock, radval, species, proj_atom, positions, 0, NPROJ, scale)
        term = lax.dot_general(beta, cblock, (((0,), (0,)), ((), ())), preferred_element_type=jnp.float32)
        return (total + term, None)
    proj, unused = lax.scan(project, jnp.zeros((NPROJ, NBANDS), jnp.float32), (miller_blocks, coeff_blocks))
    proj_b = proj.astype(jnp.bfloat16)
    mixed = jnp.dot(coupling, proj_b, preferred_element_type=jnp.float32).astype(jnp.bfloat16)

    def addback(carry, item):
        mblock, cblock = item
        radval = radial_values(mblock, radial)
        beta = make_beta(mblock, radval, species, proj_atom, positions, 0, NPROJ, scale)
        out = cblock.astype(jnp.float32) + jnp.dot(beta, mixed, preferred_element_type=jnp.float32)
        return (carry, out.astype(jnp.bfloat16))
    unused, outs = lax.scan(addback, jnp.zeros((), jnp.float32), (miller_blocks, coeff_blocks))
    return outs.reshape(NPW, NBANDS)
```

```python
import functools
import math

import jax
import jax.numpy as jnp
from jax import lax
from jax.experimental import pallas as pl
from jax.experimental.pallas import tpu as pltpu
from jax.sharding import PartitionSpec as P

NCH = 12
SHELLS = 3
COMPS = 4
MMAX = 24
LANES = 128
SPLITS = 3

SIN_POLY = (4.442882919124345, -7.308245686509103, 3.6063542184332804, -0.8461116503752865, 0.10982451642699691)
COS_POLY = (1.4142134962552289, -6.978850948563853, 5.7394603769076955, -1.8835579059892091, 0.31068802753070307)


def horner(coefs, z):
    acc = jnp.float32(coefs[-1])
    for c in coefs[-2::-1]:
        acc = acc * z + jnp.float32(c)
    return acc


def cos_sin_turns(turns):
    r = turns - jnp.round(turns)
    z = r * r
    s = horner(SIN_POLY, z) * r
    c = horner(COS_POLY, z)
    return 1.0 - s * s, s * c


def split3(x):
    hi = x.astype(jnp.bfloat16)
    rest = x - hi.astype(jnp.float32)
    mid = rest.astype(jnp.bfloat16)
    lo = (rest - mid.astype(jnp.float32)).astype(jnp.bfloat16)
    return hi, mid, lo


def nt_dot(a, b):
    return lax.dot_general(a, b, (((1,), (1,)), ((), ())), preferred_element_type=jnp.float32)


def nn_dot(a, b):
    return jnp.dot(a, b, preferred_element_type=jnp.float32)


def pack_kernel(coef_ref, mil_ref, out_ref):
    half = coef_ref.shape[1] // 2
    npw = coef_ref.shape[0]
    ct = coef_ref[...].astype(jnp.float32).T
    m = mil_ref[...].astype(jnp.float32)
    ngroups = npw // LANES
    mrows = [m[c : c + 1, g * LANES : (g + 1) * LANES] for c in range(3) for g in range(ngroups)]
    used = len(mrows)
    pad = out_ref.shape[2] - half * ngroups - used
    if pad:
        mrows.append(jnp.zeros((pad, LANES), jnp.float32))
    for h in range(2):
        rows = [ct[h * half : (h + 1) * half, g * LANES : (g + 1) * LANES] for g in range(ngroups)]
        block = jnp.concatenate(rows + mrows, axis=0).astype(jnp.bfloat16)
        out_ref[:, h] = jnp.broadcast_to(block[None], (out_ref.shape[0],) + block.shape)


def pack(coeffs, miller, ndev):
    npw, nbl = coeffs.shape
    ngroups = npw // LANES
    rows = -(-(nbl // 2 * ngroups + 3 * ngroups) // 8) * 8
    out = pl.pallas_call(
        pack_kernel,
        out_shape=jax.ShapeDtypeStruct((ndev // 2, 2, rows, LANES), jnp.bfloat16),
        name="pack",
    )(coeffs, miller)
    return out.reshape(ndev, rows, LANES)


def table_kernel(atc_ref, atr_ref, sp_ref, pos_ref, xc_ref, xr_ref, oc_ref, or_ref, *, kinds):
    natoms = sp_ref.shape[1]
    width = oc_ref.shape[2]
    per = width // SPLITS
    hi, mid, lo = split3(pos_ref[...])
    sp = sp_ref[...]
    row = lax.broadcasted_iota(jnp.int32, (width, natoms), 0) % per
    for at_ref, x_ref, o_ref in ((atc_ref, xc_ref, oc_ref), (atr_ref, xr_ref, or_ref)):
        n = at_ref.shape[0]
        pick = (lax.broadcasted_iota(jnp.int32, (n, natoms), 1) == at_ref[...]).astype(jnp.bfloat16)
        x = nt_dot(pick, hi) + nt_dot(pick, mid) + nt_dot(pick, lo)
        for c in range(3):
            x_ref[c] = jnp.broadcast_to(x[:, c : c + 1], (n, LANES))
        for s in range(SHELLS):
            kind_rows = ((row - s * kinds) == sp).astype(jnp.bfloat16)
            o_ref[s] = nt_dot(pick, kind_rows).astype(jnp.bfloat16)


def main_kernel(
    ra_ref, rb_ref, xc_ref, xr_ref, oc_ref, or_ref, rad_ref, b_hbm, own_ref, oth_ref,
    b_ref, sem, ms_ref, rads_ref, sel_ref, gc_ref, gs_ref, acc_ref, proj_ref, mix_ref,
    *, nband, scale, qscale, chunk,
):
    nga = ms_ref.shape[0]
    npw = ms_ref.shape[2]
    ngroups = npw // LANES
    half = own_ref.shape[1] // nband
    nb = 2 * own_ref.shape[1]
    nc = xc_ref.shape[1]
    nr = xr_ref.shape[1]
    nrows = b_ref.shape[0]
    qbins = rad_ref.shape[1]
    per = rads_ref.shape[1] // SPLITS

    copies = [
        pltpu.make_async_copy(b_hbm.at[pl.ds(k * chunk, chunk)], b_ref.at[pl.ds(k * chunk, chunk)], sem.at[k])
        for k in range(nrows // chunk)
    ]
    for copy in copies:
        copy.start()

    def prepare(i, carry):
        raw = ra_ref[i * nband, half * ngroups :, :].astype(jnp.float32)
        comps = [
            jnp.concatenate([raw[c * ngroups + g : c * ngroups + g + 1] for g in range(ngroups)], axis=1)
            for c in range(3)
        ]
        m = jnp.concatenate(comps + [jnp.zeros((5, npw), jnp.float32)], axis=0)
        ms_ref[i] = m
        q = (comps[0] * comps[0] + comps[1] * comps[1] + comps[2] * comps[2]) * jnp.float32(qscale)
        knot = lax.broadcasted_iota(jnp.int32, (qbins, npw), 0).astype(jnp.float32)
        hats = jnp.maximum(0.0, 1.0 - jnp.abs(q - knot))
        hi = hats.astype(jnp.bfloat16)
        lo = (hats - hi.astype(jnp.float32)).astype(jnp.bfloat16)
        table = rad_ref[...]
        r = nn_dot(table, hi) + nn_dot(table, lo)
        r = (r[0:per] + r[per : 2 * per] + r[2 * per : 3 * per]) * jnp.float32(scale)
        rads_ref[i] = jnp.concatenate(split3(r), axis=0)
        return carry

    lax.fori_loop(0, nga, prepare, 0)

    def build(i, x_ref, o_ref, n):
        rads = rads_ref[i]
        for s in range(SHELLS):
            sel_ref[s, :n] = nn_dot(o_ref[s], rads)
        m = [ms_ref[i, c : c + 1, :] for c in range(3)]
        step = 16 if n % 16 == 0 else n
        for a in range(0, n, step):
            turns = 0.0
            for c in range(3):
                x = x_ref[c, a : a + step, :]
                turns = turns + jnp.concatenate([x] * ngroups, axis=1) * m[c]
            cos, sin = cos_sin_turns(turns)
            for s in range(SHELLS):
                sel = sel_ref[s, a : a + step, :]
                gc_ref[s * n + a : s * n + a + step, :] = (sel * cos).astype(jnp.bfloat16)
                gs_ref[s * n + a : s * n + a + step, :] = (sel * sin).astype(jnp.bfloat16)

    def weights(i):
        return [ms_ref[i, c : c + 1, :] * jnp.float32(1.0 / MMAX) for c in range(3)]

    def coefs(i):
        rows = []
        for ref in (ra_ref, rb_ref):
            for j in range(nband):
                rows.append(
                    jnp.concatenate(
                        [ref[i * nband + j, g * half : (g + 1) * half, :] for g in range(ngroups)], axis=1
                    )
                )
        return jnp.concatenate(rows, axis=0)

    acc_ref[...] = jnp.zeros(acc_ref.shape, jnp.float32)

    def project(i, carry):
        build(i, xc_ref, oc_ref, nc)
        c = coefs(i)
        cf = c.astype(jnp.float32)
        w = weights(i)
        wc = jnp.concatenate([(cf * w[k]).astype(jnp.bfloat16) for k in range(3)], axis=0)
        rows = SHELLS * nc
        acc_ref[:, :nb] += nt_dot(gc_ref[:rows, :], c)
        acc_ref[:, nb:] += nt_dot(gs_ref[:rows, :], wc)
        return carry

    lax.fori_loop(0, nga, project, 0)

    for s in range(SHELLS):
        for t in range(COMPS):
            proj_ref[pl.ds(COMPS * s + t, nc, stride=NCH), :] = acc_ref[
                s * nc : (s + 1) * nc, t * nb : (t + 1) * nb
            ]
    proj = proj_ref[...].astype(jnp.bfloat16)

    for k, copy in enumerate(copies):
        copy.wait()
        mix_ref[k * chunk : (k + 1) * chunk, :] = nn_dot(b_ref[k * chunk : (k + 1) * chunk, :], proj)

    mixed = []
    for t in range(COMPS):
        m = jnp.concatenate(
            [mix_ref[pl.ds(COMPS * s + t, nr, stride=NCH), :] for s in range(SHELLS)], axis=0
        )
        mixed.append(m.T)
    m0 = mixed[0].astype(jnp.bfloat16)
    mt = jnp.concatenate(mixed[1:], axis=0).astype(jnp.bfloat16)

    def expand(i, carry):
        build(i, xr_ref, or_ref, nr)
        rows = SHELLS * nr
        y = nn_dot(m0, gc_ref[:rows, :])
        ys = nn_dot(mt, gs_ref[:rows, :])
        w = weights(i)
        for k in range(3):
            y = y + w[k] * ys[k * nb : (k + 1) * nb]
        own_ref[i] = y[: nb // 2]
        oth_ref[i] = y[nb // 2 :].astype(jnp.bfloat16)
        return carry

    lax.fori_loop(0, nga, expand, 0)


def row_chunk(count):
    for cand in range(min(count, 512), 0, -1):
        if count % cand == 0 and cand % 8 == 0:
            return cand
    return count


def finish_kernel(recv_ref, coef_ref, out_ref):
    n = recv_ref.shape[0]
    parts = []
    for h in range(2):
        def add(k, acc, h=h):
            return acc + recv_ref[k, h].astype(jnp.float32)
        parts.append(lax.fori_loop(0, n, add, jnp.zeros(recv_ref.shape[2:], jnp.float32), unroll=8))
    total = jnp.concatenate(parts, axis=0).T
    out_ref[...] = (coef_ref[...].astype(jnp.float32) + total).astype(out_ref.dtype)


def shards(coeffs, coupling, miller, species, proj_atom, positions, radial):
    nga = lax.axis_size("ga")
    nband = lax.axis_size("band")
    ndev = nga * nband
    axes = ("ga", "band")
    npw, nbl = coeffs.shape
    half = nbl // 2
    nb = nbl * nband
    nrows, ncols = coupling.shape
    nr, nc = nrows // NCH, ncols // NCH
    kinds = radial.shape[0] // SHELLS
    qbins = radial.shape[1]
    natoms = species.shape[0]
    scale = 1.0 / math.sqrt(npw * nga)
    pair = [(k, k ^ 1) for k in range(nband)]

    sent = pack(coeffs, miller, ndev)
    ra = lax.all_to_all(sent, axes, 0, 0)
    rb = lax.ppermute(ra, "band", pair)

    i = lax.axis_index("ga")
    j = lax.axis_index("band")
    atoms_c = lax.dynamic_slice_in_dim(proj_atom, j * ncols, ncols).reshape(nc, NCH)[:, :1]
    atoms_r = lax.dynamic_slice_in_dim(proj_atom, i * nrows, nrows).reshape(nr, NCH)[:, :1]
    per = -(-SHELLS * kinds // 16) * 16
    table = radial.reshape(kinds, SHELLS, qbins).transpose(1, 0, 2).reshape(SHELLS * kinds, qbins)
    table = jnp.pad(table, ((0, per - SHELLS * kinds), (0, 0)))
    hi = lax.reduce_precision(table, 8, 7)
    mid = lax.reduce_precision(table - hi, 8, 7)
    lo = table - hi - mid
    table = jnp.concatenate([hi, mid, lo], axis=0).astype(jnp.bfloat16)
    width = SPLITS * per
    xc, xr, oc, orr = pl.pallas_call(
        functools.partial(table_kernel, kinds=kinds),
        out_shape=[
            jax.ShapeDtypeStruct((3, nc, LANES), jnp.float32),
            jax.ShapeDtypeStruct((3, nr, LANES), jnp.float32),
            jax.ShapeDtypeStruct((SHELLS, nc, width), jnp.bfloat16),
            jax.ShapeDtypeStruct((SHELLS, nr, width), jnp.bfloat16),
        ],
        name="tables",
    )(atoms_c, atoms_r, species.reshape(1, natoms), positions)

    chunk = row_chunk(nrows)
    vmem = pl.BlockSpec(memory_space=pltpu.VMEM)
    nmax = max(nc, nr)
    own, other = pl.pallas_call(
        functools.partial(
            main_kernel, nband=nband, scale=scale, qscale=(qbins - 1) / (3.0 * MMAX * MMAX), chunk=chunk
        ),
        in_specs=[vmem] * 7 + [pl.BlockSpec(memory_space=pl.ANY)],
        out_specs=[vmem, vmem],
        out_shape=[
            jax.ShapeDtypeStruct((nga, nb // 2, npw), jnp.float32),
            jax.ShapeDtypeStruct((nga, nb // 2, npw), jnp.bfloat16),
        ],
        scratch_shapes=[
            pltpu.VMEM((nrows, ncols), jnp.bfloat16),
            pltpu.SemaphoreType.DMA((nrows // chunk,)),
            pltpu.VMEM((nga, 8, npw), jnp.float32),
            pltpu.VMEM((nga, width, npw), jnp.bfloat16),
            pltpu.VMEM((SHELLS, nmax, npw), jnp.float32),
            pltpu.VMEM((SHELLS * nmax, npw), jnp.bfloat16),
            pltpu.VMEM((SHELLS * nmax, npw), jnp.bfloat16),
            pltpu.VMEM((SHELLS * nc, COMPS * nb), jnp.float32),
            pltpu.VMEM((ncols, nb), jnp.float32),
            pltpu.VMEM((nrows, nb), jnp.float32),
        ],
        compiler_params=pltpu.CompilerParams(vmem_limit_bytes=56 * 1024 * 1024),
        name="apply",
    )(ra, rb, xc, xr, oc, orr, table, coupling)

    theirs = lax.ppermute(other, "band", pair)
    pairs = (own + theirs.astype(jnp.float32)).astype(jnp.bfloat16).reshape(ndev, half, npw)
    back = lax.all_to_all(pairs, axes, 0, 0).reshape(ndev // 2, 2, half, npw)
    return pl.pallas_call(
        finish_kernel,
        out_shape=jax.ShapeDtypeStruct((npw, nbl), jnp.bfloat16),
        name="finish",
    )(back, coeffs)


def solution(mesh):
    placed = (P("ga", "band"), P("ga", "band"), P(None, "ga"), P(), P(), P(), P())
    return jax.shard_map(
        shards, mesh=mesh, in_specs=placed, out_specs=P("ga", "band"), check_vma=False
    )
```

```python
import functools
import math

import jax
import jax.numpy as jnp
from jax import lax
from jax.experimental import pallas as pl
from jax.experimental.pallas import tpu as pltpu
from jax.sharding import PartitionSpec as P

NCH = 12
SHELLS = 3
COMPS = 4
MMAX = 24
LANES = 128
SPLITS = 3

SIN_POLY = (4.442882919124345, -7.308245686509103, 3.6063542184332804, -0.8461116503752865, 0.10982451642699691)
COS_POLY = (1.4142134962552289, -6.978850948563853, 5.7394603769076955, -1.8835579059892091, 0.31068802753070307)


def horner(coefs, z):
    acc = jnp.float32(coefs[-1])
    for c in coefs[-2::-1]:
        acc = acc * z + jnp.float32(c)
    return acc


def cos_sin_turns(turns):
    r = turns - jnp.round(turns)
    z = r * r
    s = horner(SIN_POLY, z) * r
    c = horner(COS_POLY, z)
    return 1.0 - s * s, s * c


def split3(x):
    hi = x.astype(jnp.bfloat16)
    rest = x - hi.astype(jnp.float32)
    mid = rest.astype(jnp.bfloat16)
    lo = (rest - mid.astype(jnp.float32)).astype(jnp.bfloat16)
    return hi, mid, lo


def nt_dot(a, b):
    return lax.dot_general(a, b, (((1,), (1,)), ((), ())), preferred_element_type=jnp.float32)


def nn_dot(a, b):
    return jnp.dot(a, b, preferred_element_type=jnp.float32)


def pack_kernel(coef_ref, mil_ref, out_ref):
    half = coef_ref.shape[0] // 2
    ngroups = coef_ref.shape[1] // LANES
    m = mil_ref[...].astype(jnp.float32)
    mrows = [m[c : c + 1, g * LANES : (g + 1) * LANES] for c in range(3) for g in range(ngroups)]
    pad = out_ref.shape[2] - half * ngroups - len(mrows)
    if pad:
        mrows.append(jnp.zeros((pad, LANES), jnp.float32))
    mblock = jnp.concatenate(mrows, axis=0).astype(jnp.bfloat16)
    for h in range(2):
        rows = [
            coef_ref[h * half : (h + 1) * half, g * LANES : (g + 1) * LANES] for g in range(ngroups)
        ]
        block = jnp.concatenate(rows + [mblock], axis=0)
        for d in range(out_ref.shape[0]):
            out_ref[d, h] = block


def pack(coeffs_t, miller, ndev):
    nbl, npw = coeffs_t.shape
    ngroups = npw // LANES
    rows = -(-(nbl // 2 * ngroups + 3 * ngroups) // 8) * 8
    out = pl.pallas_call(
        pack_kernel,
        out_shape=jax.ShapeDtypeStruct((ndev // 2, 2, rows, LANES), jnp.bfloat16),
        name="pack",
    )(coeffs_t, miller)
    return out.reshape(ndev, rows, LANES)


def table_kernel(atc_ref, atr_ref, sp_ref, pos_ref, xc_ref, xr_ref, oc_ref, or_ref, *, kinds):
    natoms = sp_ref.shape[1]
    width = oc_ref.shape[2]
    per = width // SPLITS
    hi, mid, lo = split3(pos_ref[...])
    sp = sp_ref[...]
    row = lax.broadcasted_iota(jnp.int32, (width, natoms), 0) % per
    for at_ref, x_ref, o_ref in ((atc_ref, xc_ref, oc_ref), (atr_ref, xr_ref, or_ref)):
        n = at_ref.shape[0]
        pick = (lax.broadcasted_iota(jnp.int32, (n, natoms), 1) == at_ref[...]).astype(jnp.bfloat16)
        x = nt_dot(pick, hi) + nt_dot(pick, mid) + nt_dot(pick, lo)
        for c in range(3):
            x_ref[c] = jnp.broadcast_to(x[:, c : c + 1], (n, LANES))
        for s in range(SHELLS):
            kind_rows = ((row - s * kinds) == sp).astype(jnp.bfloat16)
            o_ref[s] = nt_dot(pick, kind_rows).astype(jnp.bfloat16)


def main_kernel(
    ra_ref, rb_ref, xc_ref, xr_ref, oc_ref, or_ref, rad_ref, b_hbm, own_ref, oth_ref,
    b_ref, sem, ms_ref, rads_ref, sel_ref, gca_ref, gsa_ref, cf_ref, acc_ref, proj_ref, mix_ref,
    gcc_ref, gsc_ref,
    *, nband, scale, qscale, chunk, group,
):
    nga = ms_ref.shape[0]
    npw = ms_ref.shape[2]
    ngroups = npw // LANES
    half = own_ref.shape[1] // nband
    nb = 2 * own_ref.shape[1]
    nc = xc_ref.shape[1]
    nr = xr_ref.shape[1]
    nrows = b_ref.shape[0]
    qbins = rad_ref.shape[1]
    per = rads_ref.shape[1] // SPLITS
    nsteps = nga // group

    copies = [
        pltpu.make_async_copy(b_hbm.at[pl.ds(k * chunk, chunk)], b_ref.at[pl.ds(k * chunk, chunk)], sem.at[k])
        for k in range(nrows // chunk)
    ]
    for copy in copies:
        copy.start()

    def prepare(i):
        raw = ra_ref[i * nband, half * ngroups :, :].astype(jnp.float32)
        comps = [
            jnp.concatenate([raw[c * ngroups + g : c * ngroups + g + 1] for g in range(ngroups)], axis=1)
            for c in range(3)
        ]
        for c in range(3):
            ms_ref[i, c : c + 1, :] = comps[c]
        q = (comps[0] * comps[0] + comps[1] * comps[1] + comps[2] * comps[2]) * jnp.float32(qscale)
        knot = lax.broadcasted_iota(jnp.int32, (qbins, npw), 0).astype(jnp.float32)
        hats = jnp.maximum(0.0, 1.0 - jnp.abs(q - knot))
        hi = hats.astype(jnp.bfloat16)
        lo = (hats - hi.astype(jnp.float32)).astype(jnp.bfloat16)
        table = rad_ref[...]
        r = nn_dot(table, hi) + nn_dot(table, lo)
        r = (r[0:per] + r[per : 2 * per] + r[2 * per : 3 * per]) * jnp.float32(scale)
        rads_ref[i] = jnp.concatenate(split3(r), axis=0)

    def build(i, x_ref, o_ref, n, sel, put):
        rads = rads_ref[i]
        for s in range(SHELLS):
            sel[s, :n] = nn_dot(o_ref[s], rads)
        m = [ms_ref[i, c : c + 1, :] for c in range(3)]
        step = 16 if n % 16 == 0 else n
        for a in range(0, n, step):
            turns = 0.0
            for c in range(3):
                x = x_ref[c, a : a + step, :]
                turns = turns + jnp.concatenate([x] * ngroups, axis=1) * m[c]
            cos, sin = cos_sin_turns(turns)
            for s in range(SHELLS):
                v = sel[s, a : a + step, :]
                put(s * n + a, step, (v * cos).astype(jnp.bfloat16), (v * sin).astype(jnp.bfloat16))

    def weights(i):
        return [ms_ref[i, c : c + 1, :] * jnp.float32(1.0 / MMAX) for c in range(3)]

    def coefs(i):
        rows = []
        for ref in (ra_ref, rb_ref):
            for j in range(nband):
                rows.append(
                    jnp.concatenate(
                        [ref[i * nband + j, g * half : (g + 1) * half, :] for g in range(ngroups)], axis=1
                    )
                )
        return jnp.concatenate(rows, axis=0)

    def stage(step, slot):
        for e in range(group):
            i = step * group + e
            lanes = slice(e * npw, (e + 1) * npw)

            def put(row, count, c, s, lanes=lanes):
                gca_ref[slot, row : row + count, lanes] = c
                gsa_ref[slot, row : row + count, lanes] = s

            prepare(i)
            build(i, xc_ref, oc_ref, nc, sel_ref.at[slot], put)
            c = coefs(i)
            cf = c.astype(jnp.float32)
            w = weights(i)
            cf_ref[slot, :nb, lanes] = c
            for k in range(3):
                cf_ref[slot, (k + 1) * nb : (k + 2) * nb, lanes] = (cf * w[k]).astype(jnp.bfloat16)

    def consume(slot):
        acc_ref[:, :nb] += nt_dot(gca_ref[slot], cf_ref[slot, :nb])
        acc_ref[:, nb:] += nt_dot(gsa_ref[slot], cf_ref[slot, nb:])

    def clear(k, carry):
        acc_ref[pl.ds(pl.multiple_of(k * nc, 8), nc), :] = jnp.zeros((nc, acc_ref.shape[1]), jnp.float32)
        return carry

    lax.fori_loop(0, SHELLS, clear, 0)
    stage(0, 0)
    if nsteps <= 8:
        for step in range(1, nsteps):
            stage(step, step % 2)
            consume((step - 1) % 2)
    else:
        def body(step, carry):
            slot = step % 2
            stage(step, slot)
            consume(1 - slot)
            return carry

        lax.fori_loop(1, nsteps, body, 0)
    def rebuild(i, slot):
        def put(row, count, c, s):
            gcc_ref[i, row : row + count, :] = c
            gsc_ref[i, row : row + count, :] = s

        build(i, xr_ref, or_ref, nr, sel_ref.at[slot], put)

    early = 4 if nga <= 16 else 0
    for i in range(early):
        rebuild(i, i % 2)
    consume((nsteps - 1) % 2)

    for s in range(SHELLS):
        for t in range(COMPS):
            proj_ref[pl.ds(COMPS * s + t, nc, stride=NCH), :] = acc_ref[
                s * nc : (s + 1) * nc, t * nb : (t + 1) * nb
            ]
    proj = proj_ref[...].astype(jnp.bfloat16)

    def multiply(first, count):
        mix_ref[first : first + count, :] = nn_dot(b_ref[first : first + count, :], proj)

    for copy in copies:
        copy.wait()
    nmul = nrows // chunk
    if nga <= 16:
        for k in range(nmul):
            multiply(k * chunk, chunk)
            for i in range(early + k * (nga - early) // nmul, early + (k + 1) * (nga - early) // nmul):
                rebuild(i, i % 2)
    else:
        for k in range(nmul):
            multiply(k * chunk, chunk)

        def again(i, carry):
            rebuild(i, i % 2)
            return carry

        lax.fori_loop(0, nga, again, 0)

    mixed = []
    for t in range(COMPS):
        m = jnp.concatenate(
            [mix_ref[pl.ds(COMPS * s + t, nr, stride=NCH), :] for s in range(SHELLS)], axis=0
        )
        mixed.append(m.T)
    m0 = mixed[0].astype(jnp.bfloat16)
    mt = jnp.concatenate(mixed[1:], axis=0).astype(jnp.bfloat16)

    def expand(i):
        y = nn_dot(m0, gcc_ref[i])
        ys = nn_dot(mt, gsc_ref[i])
        w = weights(i)
        for k in range(3):
            y = y + w[k] * ys[k * nb : (k + 1) * nb]
        own_ref[i] = y[: nb // 2]
        oth_ref[i] = y[nb // 2 :].astype(jnp.bfloat16)

    if nga <= 16:
        for i in range(nga):
            expand(i)
    else:
        def body(i, carry):
            expand(i)
            return carry

        lax.fori_loop(0, nga, body, 0)


def row_chunk(count):
    for cand in range(min(count, 256), 0, -1):
        if count % cand == 0 and cand % 8 == 0:
            return cand
    return count


def finish_kernel(recv_ref, coef_ref, out_ref):
    n = recv_ref.shape[0]
    parts = []
    for h in range(2):
        def add(k, acc, h=h):
            return acc + recv_ref[k, h].astype(jnp.float32)
        parts.append(lax.fori_loop(0, n, add, jnp.zeros(recv_ref.shape[2:], jnp.float32), unroll=8))
    total = jnp.concatenate(parts, axis=0)
    out_ref[...] = (coef_ref[...].astype(jnp.float32) + total).astype(out_ref.dtype)


def shards(coeffs, coupling, miller, species, proj_atom, positions, radial):
    nga = lax.axis_size("ga")
    nband = lax.axis_size("band")
    ndev = nga * nband
    axes = ("ga", "band")
    npw, nbl = coeffs.shape
    half = nbl // 2
    nb = nbl * nband
    nrows, ncols = coupling.shape
    nr, nc = nrows // NCH, ncols // NCH
    kinds = radial.shape[0] // SHELLS
    qbins = radial.shape[1]
    natoms = species.shape[0]
    scale = 1.0 / math.sqrt(npw * nga)
    pair = [(k, k ^ 1) for k in range(nband)]

    coeffs_t = coeffs.T
    sent = pack(coeffs_t, miller, ndev)
    ra = lax.all_to_all(sent, axes, 0, 0)
    i = lax.axis_index("ga")
    j = lax.axis_index("band")
    atoms_c = lax.dynamic_slice_in_dim(proj_atom, j * ncols, ncols).reshape(nc, NCH)[:, :1]
    atoms_r = lax.dynamic_slice_in_dim(proj_atom, i * nrows, nrows).reshape(nr, NCH)[:, :1]
    per = -(-SHELLS * kinds // 16) * 16
    table = radial.reshape(kinds, SHELLS, qbins).transpose(1, 0, 2).reshape(SHELLS * kinds, qbins)
    table = jnp.pad(table, ((0, per - SHELLS * kinds), (0, 0)))
    hi = lax.reduce_precision(table, 8, 7)
    mid = lax.reduce_precision(table - hi, 8, 7)
    lo = table - hi - mid
    table = jnp.concatenate([hi, mid, lo], axis=0).astype(jnp.bfloat16)
    width = SPLITS * per
    xc, xr, oc, orr = pl.pallas_call(
        functools.partial(table_kernel, kinds=kinds),
        out_shape=[
            jax.ShapeDtypeStruct((3, nc, LANES), jnp.float32),
            jax.ShapeDtypeStruct((3, nr, LANES), jnp.float32),
            jax.ShapeDtypeStruct((SHELLS, nc, width), jnp.bfloat16),
            jax.ShapeDtypeStruct((SHELLS, nr, width), jnp.bfloat16),
        ],
        cost_estimate=pl.CostEstimate(flops=10**9, transcendentals=0, bytes_accessed=10**6),
        compiler_params=pltpu.CompilerParams(vmem_limit_bytes=16 * 1024 * 1024),
        name="tables",
    )(atoms_c, atoms_r, species.reshape(1, natoms), positions)

    ra, table, xc, xr, oc, orr = lax.optimization_barrier((ra, table, xc, xr, oc, orr))
    rb = lax.ppermute(ra, "band", pair)

    chunk = row_chunk(nrows)
    vmem = pl.BlockSpec(memory_space=pltpu.VMEM)
    nmax = max(nc, nr)
    group = 2 if nga % 2 == 0 else 1
    own, other = pl.pallas_call(
        functools.partial(
            main_kernel, nband=nband, scale=scale, qscale=(qbins - 1) / (3.0 * MMAX * MMAX), chunk=chunk,
            group=group,
        ),
        in_specs=[vmem] * 7 + [pl.BlockSpec(memory_space=pl.ANY)],
        out_specs=[vmem, vmem],
        out_shape=[
            jax.ShapeDtypeStruct((nga, nb // 2, npw), jnp.float32),
            jax.ShapeDtypeStruct((nga, nb // 2, npw), jnp.bfloat16),
        ],
        scratch_shapes=[
            pltpu.VMEM((nrows, ncols), jnp.bfloat16),
            pltpu.SemaphoreType.DMA((nrows // chunk,)),
            pltpu.VMEM((nga, 8, npw), jnp.float32),
            pltpu.VMEM((nga, width, npw), jnp.bfloat16),
            pltpu.VMEM((2, SHELLS, nmax, npw), jnp.float32),
            pltpu.VMEM((2, SHELLS * nc, group * npw), jnp.bfloat16),
            pltpu.VMEM((2, SHELLS * nc, group * npw), jnp.bfloat16),
            pltpu.VMEM((2, COMPS * nb, group * npw), jnp.bfloat16),
            pltpu.VMEM((SHELLS * nc, COMPS * nb), jnp.float32),
            pltpu.VMEM((ncols, nb), jnp.float32),
            pltpu.VMEM((nrows, nb), jnp.float32),
            pltpu.VMEM((nga, SHELLS * nr, npw), jnp.bfloat16),
            pltpu.VMEM((nga, SHELLS * nr, npw), jnp.bfloat16),
        ],
        compiler_params=pltpu.CompilerParams(vmem_limit_bytes=50 * 1024 * 1024),
        name="apply",
    )(ra, rb, xc, xr, oc, orr, table, coupling)

    theirs = lax.ppermute(other, "band", pair)
    pairs = (own + theirs.astype(jnp.float32)).astype(jnp.bfloat16).reshape(ndev, half, npw)
    back = lax.all_to_all(pairs, axes, 0, 0).reshape(ndev // 2, 2, half, npw)
    return pl.pallas_call(
        finish_kernel,
        out_shape=jax.ShapeDtypeStruct((nbl, npw), jnp.bfloat16),
        compiler_params=pltpu.CompilerParams(vmem_limit_bytes=16 * 1024 * 1024),
        name="finish",
    )(back, coeffs_t).T


def solution(mesh):
    placed = (P("ga", "band"), P("ga", "band"), P(None, "ga"), P(), P(), P(), P())
    return jax.shard_map(
        shards, mesh=mesh, in_specs=placed, out_specs=P("ga", "band"), check_vma=False
    )
```

```python
import functools
import math

import jax
import jax.numpy as jnp
from jax import lax
from jax.experimental import pallas as pl
from jax.experimental.pallas import tpu as pltpu
from jax.sharding import PartitionSpec as P

NCH = 12
SHELLS = 3
COMPS = 4
MMAX = 24
LANES = 128
SPLITS = 3
EARLY = 2

SIN_POLY = (4.442882919124345, -7.308245686509103, 3.6063542184332804, -0.8461116503752865, 0.10982451642699691)
COS_POLY = (1.4142134962552289, -6.978850948563853, 5.7394603769076955, -1.8835579059892091, 0.31068802753070307)


def horner(coefs, z):
    acc = jnp.float32(coefs[-1])
    for c in coefs[-2::-1]:
        acc = acc * z + jnp.float32(c)
    return acc


def cos_sin_turns(turns):
    r = turns - jnp.round(turns)
    z = r * r
    s = horner(SIN_POLY, z) * r
    c = horner(COS_POLY, z)
    return 1.0 - s * s, s * c


def split3(x):
    hi = x.astype(jnp.bfloat16)
    rest = x - hi.astype(jnp.float32)
    mid = rest.astype(jnp.bfloat16)
    lo = (rest - mid.astype(jnp.float32)).astype(jnp.bfloat16)
    return hi, mid, lo


def nt_dot(a, b):
    return lax.dot_general(a, b, (((1,), (1,)), ((), ())), preferred_element_type=jnp.float32)


def nn_dot(a, b):
    return jnp.dot(a, b, preferred_element_type=jnp.float32)


def pack_kernel(coef_ref, mil_ref, out_ref):
    half = coef_ref.shape[0] // 2
    ngroups = coef_ref.shape[1] // LANES
    m = mil_ref[...].astype(jnp.float32)
    mrows = [m[c : c + 1, g * LANES : (g + 1) * LANES] for c in range(3) for g in range(ngroups)]
    pad = out_ref.shape[2] - half * ngroups - len(mrows)
    if pad:
        mrows.append(jnp.zeros((pad, LANES), jnp.float32))
    mblock = jnp.concatenate(mrows, axis=0).astype(jnp.bfloat16)
    for h in range(2):
        rows = [
            coef_ref[h * half : (h + 1) * half, g * LANES : (g + 1) * LANES] for g in range(ngroups)
        ]
        block = jnp.concatenate(rows + [mblock], axis=0)
        for d in range(out_ref.shape[0]):
            out_ref[d, h] = block


def pack(coeffs_t, miller, ndev):
    nbl, npw = coeffs_t.shape
    ngroups = npw // LANES
    rows = -(-(nbl // 2 * ngroups + 3 * ngroups) // 8) * 8
    out = pl.pallas_call(
        pack_kernel,
        out_shape=jax.ShapeDtypeStruct((ndev // 2, 2, rows, LANES), jnp.bfloat16),
        name="pack",
    )(coeffs_t, miller)
    return out.reshape(ndev, rows, LANES)


def table_kernel(atc_ref, atr_ref, sp_ref, pos_ref, xc_ref, xr_ref, oc_ref, or_ref, *, kinds):
    natoms = sp_ref.shape[1]
    width = oc_ref.shape[2]
    per = width // SPLITS
    hi, mid, lo = split3(pos_ref[...])
    sp = sp_ref[...]
    row = lax.broadcasted_iota(jnp.int32, (width, natoms), 0) % per
    for at_ref, x_ref, o_ref in ((atc_ref, xc_ref, oc_ref), (atr_ref, xr_ref, or_ref)):
        n = at_ref.shape[0]
        pick = (lax.broadcasted_iota(jnp.int32, (n, natoms), 1) == at_ref[...]).astype(jnp.bfloat16)
        x = nt_dot(pick, hi) + nt_dot(pick, mid) + nt_dot(pick, lo)
        for c in range(3):
            x_ref[c] = jnp.broadcast_to(x[:, c : c + 1], (n, LANES))
        for s in range(SHELLS):
            kind_rows = ((row - s * kinds) == sp).astype(jnp.bfloat16)
            o_ref[s] = nt_dot(pick, kind_rows).astype(jnp.bfloat16)


def build(i, x_ref, o_ref, rads_ref, ms_ref, sel, put):
    n = x_ref.shape[1]
    ngroups = ms_ref.shape[2] // LANES
    step = 16 if n % 16 == 0 else n
    blocks = 4 if n % 64 == 0 else 1

    def select(s):
        sel[s, :n] = nn_dot(o_ref[s], rads_ref[i])

    def rows(first):
        m = [ms_ref[i, c : c + 1, :] for c in range(3)]
        for a in range(first, first + n // blocks, step):
            turns = 0.0
            for c in range(3):
                x = x_ref[c, a : a + step, :]
                turns = turns + jnp.concatenate([x] * ngroups, axis=1) * m[c]
            cos, sin = cos_sin_turns(turns)
            for s in range(SHELLS):
                v = sel[s, a : a + step, :]
                put(s * n + a, step, (v * cos).astype(jnp.bfloat16), (v * sin).astype(jnp.bfloat16))

    return [functools.partial(select, s) for s in range(SHELLS)] + [
        functools.partial(rows, k * (n // blocks)) for k in range(blocks)
    ]


def mingle(first, second):
    done = 0
    for k, piece in enumerate(first):
        piece()
        upto = (k + 1) * len(second) // len(first)
        for other in second[done:upto]:
            other()
        done = upto


def unrolled(count):
    return count <= 16


def early_kernel(
    ra_ref, xc_ref, xr_ref, oc_ref, or_ref, rad_ref,
    ms_ref, rads_ref, gca_ref, gsa_ref, gcc_ref, gsc_ref, sel_ref,
    *, nband, half, scale, qscale
):
    nga, _, npw = ms_ref.shape
    ngroups = npw // LANES
    qbins = rad_ref.shape[1]
    per = rads_ref.shape[1] // SPLITS
    first = half * ngroups

    def prepare(i):
        raw = ra_ref[i * nband, first:, :].astype(jnp.float32)
        comps = [
            jnp.concatenate([raw[c * ngroups + g : c * ngroups + g + 1] for g in range(ngroups)], axis=1)
            for c in range(3)
        ]
        for c in range(3):
            ms_ref[i, c : c + 1, :] = comps[c]
        q = (comps[0] * comps[0] + comps[1] * comps[1] + comps[2] * comps[2]) * jnp.float32(qscale)
        knot = lax.broadcasted_iota(jnp.int32, (qbins, npw), 0).astype(jnp.float32)
        hats = jnp.maximum(0.0, 1.0 - jnp.abs(q - knot))
        hi = hats.astype(jnp.bfloat16)
        lo = (hats - hi.astype(jnp.float32)).astype(jnp.bfloat16)
        table = rad_ref[...]
        r = nn_dot(table, hi) + nn_dot(table, lo)
        r = (r[0:per] + r[per : 2 * per] + r[2 * per : 3 * per]) * jnp.float32(scale)
        rads_ref[i] = jnp.concatenate(split3(r), axis=0)

    if unrolled(nga):
        for i in range(nga):
            prepare(i)
    else:
        def body(i, carry):
            prepare(i)
            return carry

        lax.fori_loop(0, nga, body, 0)

    def rebuild(i, slot):
        def put(row, count, c, s):
            gcc_ref[i, row : row + count, :] = c
            gsc_ref[i, row : row + count, :] = s

        return build(i, xr_ref, or_ref, rads_ref, ms_ref, sel_ref.at[slot], put)

    def start(i, slot):
        lanes = slice(i * npw, (i + 1) * npw)

        def put(row, count, c, s):
            gca_ref[row : row + count, lanes] = c
            gsa_ref[row : row + count, lanes] = s

        return build(i, xc_ref, oc_ref, rads_ref, ms_ref, sel_ref.at[slot], put)

    for i in range(gca_ref.shape[1] // npw):
        mingle(start(i, i % 2), [])
    for i in range(gcc_ref.shape[0]):
        mingle(rebuild(i, i % 2), [])


def main_kernel(
    ra_ref, rb_ref, xc_ref, xr_ref, oc_ref, or_ref, ms_ref, rads_ref, gc0_ref, gs0_ref,
    gce_ref, gse_ref, b_hbm,
    own_ref, oth_ref, b_ref, sem, sel_ref, gca_ref, gsa_ref, cf_ref, acc_ref, proj_ref, mix_ref,
    gcc_ref, gsc_ref,
    *, nband, chunk, group,
):
    nga = ms_ref.shape[0]
    npw = ms_ref.shape[2]
    ngroups = npw // LANES
    half = own_ref.shape[1] // nband
    nb = 2 * own_ref.shape[1]
    nc = xc_ref.shape[1]
    nr = xr_ref.shape[1]
    nrows = b_ref.shape[0]
    early = gce_ref.shape[0] if unrolled(nga) else 0
    nsteps = nga // group

    copies = [
        pltpu.make_async_copy(b_hbm.at[pl.ds(k * chunk, chunk)], b_ref.at[pl.ds(k * chunk, chunk)], sem.at[k])
        for k in range(nrows // chunk)
    ]
    for copy in copies:
        copy.start()

    def weights(i):
        return [ms_ref[i, c : c + 1, :] * jnp.float32(1.0 / MMAX) for c in range(3)]

    def coefs(i):
        rows = []
        for ref in (ra_ref, rb_ref):
            for j in range(nband):
                rows.append(
                    jnp.concatenate(
                        [ref[i * nband + j, g * half : (g + 1) * half, :] for g in range(ngroups)], axis=1
                    )
                )
        return jnp.concatenate(rows, axis=0)

    def stage(step, slot, ready=False):
        pieces = []
        for e in range(group):
            i = step * group + e
            lanes = slice(e * npw, (e + 1) * npw)

            def put(row, count, c, s, lanes=lanes):
                gca_ref[slot, row : row + count, lanes] = c
                gsa_ref[slot, row : row + count, lanes] = s

            def scaled(i=i, lanes=lanes):
                c = coefs(i)
                cf = c.astype(jnp.float32)
                w = weights(i)
                cf_ref[slot, :nb, lanes] = c
                for k in range(3):
                    cf_ref[slot, (k + 1) * nb : (k + 2) * nb, lanes] = (cf * w[k]).astype(jnp.bfloat16)

            if not ready:
                pieces.extend(build(i, xc_ref, oc_ref, rads_ref, ms_ref, sel_ref.at[slot], put))
            pieces.append(scaled)
        return pieces

    def consume(gc, gs, slot):
        def cosines(s):
            rows = slice(s * nc, (s + 1) * nc)
            acc_ref[rows, :nb] += nt_dot(gc[rows, :], cf_ref[slot, :nb])

        def sines(s):
            rows = slice(s * nc, (s + 1) * nc)
            acc_ref[rows, nb:] += nt_dot(gs[rows, :], cf_ref[slot, nb:])

        return [functools.partial(f, s) for s in range(SHELLS) for f in (cosines, sines)]

    def consume_slot(slot):
        return consume(gca_ref.at[slot], gsa_ref.at[slot], slot)

    def clear(k, carry):
        acc_ref[pl.ds(pl.multiple_of(k * nc, 8), nc), :] = jnp.zeros((nc, acc_ref.shape[1]), jnp.float32)
        return carry

    lax.fori_loop(0, SHELLS, clear, 0)
    mingle(stage(0, 0, ready=True), [])
    last = consume(gc0_ref, gs0_ref, 0)
    if nsteps <= 8:
        for step in range(1, nsteps):
            mingle(stage(step, step % 2), last)
            last = consume_slot(step % 2)
    else:
        mingle(stage(1, 1), last)

        def body(step, carry):
            slot = step % 2
            mingle(stage(step, slot), consume_slot(1 - slot))
            return carry

        lax.fori_loop(2, nsteps, body, 0)
        last = consume_slot((nsteps - 1) % 2)
    mingle([lambda: None], last)

    for s in range(SHELLS):
        for t in range(COMPS):
            proj_ref[pl.ds(COMPS * s + t, nc, stride=NCH), :] = acc_ref[
                s * nc : (s + 1) * nc, t * nb : (t + 1) * nb
            ]
    proj = proj_ref[...].astype(jnp.bfloat16)

    def rebuild(i, slot):
        def put(row, count, c, s):
            gcc_ref[i - early, row : row + count, :] = c
            gsc_ref[i - early, row : row + count, :] = s

        return build(i, xr_ref, or_ref, rads_ref, ms_ref, sel_ref.at[slot], put)

    def multiply(first, count):
        mix_ref[first : first + count, :] = nn_dot(b_ref[first : first + count, :], proj)

    for copy in copies:
        copy.wait()
    nmul = nrows // chunk
    if unrolled(nga):
        for k in range(nmul):
            multiply(k * chunk, chunk)
            for i in range(early + k * (nga - early) // nmul, early + (k + 1) * (nga - early) // nmul):
                mingle(rebuild(i, i % 2), [])
    else:
        for k in range(nmul):
            multiply(k * chunk, chunk)

        def again(i, carry):
            mingle(rebuild(i, i % 2), [])
            return carry

        lax.fori_loop(0, nga, again, 0)

    mixed = []
    for t in range(COMPS):
        m = jnp.concatenate(
            [mix_ref[pl.ds(COMPS * s + t, nr, stride=NCH), :] for s in range(SHELLS)], axis=0
        )
        mixed.append(m.T)
    m0 = mixed[0].astype(jnp.bfloat16)
    mt = jnp.concatenate(mixed[1:], axis=0).astype(jnp.bfloat16)

    def expand(i):
        here = unrolled(nga) and i < early
        y = nn_dot(m0, gce_ref[i] if here else gcc_ref[i - early])
        ys = nn_dot(mt, gse_ref[i] if here else gsc_ref[i - early])
        w = weights(i)
        for k in range(3):
            y = y + w[k] * ys[k * nb : (k + 1) * nb]
        own_ref[i] = y[: nb // 2]
        oth_ref[i] = y[nb // 2 :].astype(jnp.bfloat16)

    if unrolled(nga):
        for i in range(nga):
            expand(i)
    else:
        def body(i, carry):
            expand(i)
            return carry

        lax.fori_loop(0, nga, body, 0)


def row_chunk(count):
    for cand in range(min(count, 256), 0, -1):
        if count % cand == 0 and cand % 8 == 0:
            return cand
    return count


def finish_kernel(recv_ref, coef_ref, out_ref):
    n = recv_ref.shape[0]
    parts = []
    for h in range(2):
        def add(k, acc, h=h):
            return acc + recv_ref[k, h].astype(jnp.float32)
        parts.append(lax.fori_loop(0, n, add, jnp.zeros(recv_ref.shape[2:], jnp.float32), unroll=8))
    total = jnp.concatenate(parts, axis=0)
    out_ref[...] = (coef_ref[...].astype(jnp.float32) + total).astype(out_ref.dtype)


def shards(coeffs, coupling, miller, species, proj_atom, positions, radial):
    nga = lax.axis_size("ga")
    nband = lax.axis_size("band")
    ndev = nga * nband
    axes = ("ga", "band")
    npw, nbl = coeffs.shape
    half = nbl // 2
    nb = nbl * nband
    nrows, ncols = coupling.shape
    nr, nc = nrows // NCH, ncols // NCH
    kinds = radial.shape[0] // SHELLS
    qbins = radial.shape[1]
    natoms = species.shape[0]
    scale = 1.0 / math.sqrt(npw * nga)
    pair = [(k, k ^ 1) for k in range(nband)]

    coeffs_t = coeffs.T
    sent = pack(coeffs_t, miller, ndev)
    ra = lax.all_to_all(sent, axes, 0, 0)
    i = lax.axis_index("ga")
    j = lax.axis_index("band")
    atoms_c = lax.dynamic_slice_in_dim(proj_atom, j * ncols, ncols).reshape(nc, NCH)[:, :1]
    atoms_r = lax.dynamic_slice_in_dim(proj_atom, i * nrows, nrows).reshape(nr, NCH)[:, :1]
    per = -(-SHELLS * kinds // 16) * 16
    table = radial.reshape(kinds, SHELLS, qbins).transpose(1, 0, 2).reshape(SHELLS * kinds, qbins)
    table = jnp.pad(table, ((0, per - SHELLS * kinds), (0, 0)))
    hi = lax.reduce_precision(table, 8, 7)
    mid = lax.reduce_precision(table - hi, 8, 7)
    lo = table - hi - mid
    table = jnp.concatenate([hi, mid, lo], axis=0).astype(jnp.bfloat16)
    width = SPLITS * per
    xc, xr, oc, orr = pl.pallas_call(
        functools.partial(table_kernel, kinds=kinds),
        out_shape=[
            jax.ShapeDtypeStruct((3, nc, LANES), jnp.float32),
            jax.ShapeDtypeStruct((3, nr, LANES), jnp.float32),
            jax.ShapeDtypeStruct((SHELLS, nc, width), jnp.bfloat16),
            jax.ShapeDtypeStruct((SHELLS, nr, width), jnp.bfloat16),
        ],
        cost_estimate=pl.CostEstimate(flops=10**9, transcendentals=0, bytes_accessed=10**6),
        compiler_params=pltpu.CompilerParams(vmem_limit_bytes=16 * 1024 * 1024),
        name="tables",
    )(atoms_c, atoms_r, species.reshape(1, natoms), positions)

    ra, table, xc, xr, oc, orr = lax.optimization_barrier((ra, table, xc, xr, oc, orr))
    rb = lax.ppermute(ra, "band", pair)

    chunk = row_chunk(nrows)
    vmem = pl.BlockSpec(memory_space=pltpu.VMEM)
    nmax = max(nc, nr)
    group = 2 if nga % 2 == 0 else 1
    early = min(EARLY, nga // 2)
    kept = nga - early if unrolled(nga) else nga
    ms, rads, gc0, gs0, gce, gse = pl.pallas_call(
        functools.partial(
            early_kernel, nband=nband, half=half, scale=scale, qscale=(qbins - 1) / (3.0 * MMAX * MMAX)
        ),
        out_shape=[
            jax.ShapeDtypeStruct((nga, 8, npw), jnp.float32),
            jax.ShapeDtypeStruct((nga, width, npw), jnp.bfloat16),
            jax.ShapeDtypeStruct((SHELLS * nc, group * npw), jnp.bfloat16),
            jax.ShapeDtypeStruct((SHELLS * nc, group * npw), jnp.bfloat16),
            jax.ShapeDtypeStruct((early, SHELLS * nr, npw), jnp.bfloat16),
            jax.ShapeDtypeStruct((early, SHELLS * nr, npw), jnp.bfloat16),
        ],
        scratch_shapes=[pltpu.VMEM((2, SHELLS, nmax, npw), jnp.float32)],
        compiler_params=pltpu.CompilerParams(vmem_limit_bytes=32 * 1024 * 1024),
        cost_estimate=pl.CostEstimate(flops=10**9, transcendentals=0, bytes_accessed=10**6),
        name="early",
    )(ra, xc, xr, oc, orr, table)
    own, other = pl.pallas_call(
        functools.partial(main_kernel, nband=nband, chunk=chunk, group=group),
        in_specs=[vmem] * 12 + [pl.BlockSpec(memory_space=pl.ANY)],
        out_specs=[vmem, vmem],
        out_shape=[
            jax.ShapeDtypeStruct((nga, nb // 2, npw), jnp.float32),
            jax.ShapeDtypeStruct((nga, nb // 2, npw), jnp.bfloat16),
        ],
        scratch_shapes=[
            pltpu.VMEM((nrows, ncols), jnp.bfloat16),
            pltpu.SemaphoreType.DMA((nrows // chunk,)),
            pltpu.VMEM((2, SHELLS, nmax, npw), jnp.float32),
            pltpu.VMEM((2, SHELLS * nc, group * npw), jnp.bfloat16),
            pltpu.VMEM((2, SHELLS * nc, group * npw), jnp.bfloat16),
            pltpu.VMEM((2, COMPS * nb, group * npw), jnp.bfloat16),
            pltpu.VMEM((SHELLS * nc, COMPS * nb), jnp.float32),
            pltpu.VMEM((ncols, nb), jnp.float32),
            pltpu.VMEM((nrows, nb), jnp.float32),
            pltpu.VMEM((kept, SHELLS * nr, npw), jnp.bfloat16),
            pltpu.VMEM((kept, SHELLS * nr, npw), jnp.bfloat16),
        ],
        compiler_params=pltpu.CompilerParams(vmem_limit_bytes=46 * 1024 * 1024),
        name="apply",
    )(ra, rb, xc, xr, oc, orr, ms, rads, gc0, gs0, gce, gse, coupling)

    theirs = lax.ppermute(other, "band", pair)
    pairs = (own + theirs.astype(jnp.float32)).astype(jnp.bfloat16).reshape(ndev, half, npw)
    back = lax.all_to_all(pairs, axes, 0, 0).reshape(ndev // 2, 2, half, npw)
    return pl.pallas_call(
        finish_kernel,
        out_shape=jax.ShapeDtypeStruct((nbl, npw), jnp.bfloat16),
        compiler_params=pltpu.CompilerParams(vmem_limit_bytes=16 * 1024 * 1024),
        name="finish",
    )(back, coeffs_t).T


def solution(mesh):
    placed = (P("ga", "band"), P("ga", "band"), P(None, "ga"), P(), P(), P(), P())
    return jax.shard_map(
        shards, mesh=mesh, in_specs=placed, out_specs=P("ga", "band"), check_vma=False
    )
```

```python
import functools
import math

import jax
import jax.numpy as jnp
from jax import lax
from jax.experimental import pallas as pl
from jax.experimental.pallas import tpu as pltpu
from jax.sharding import PartitionSpec as P

NCH = 12
SHELLS = 3
COMPS = 4
MMAX = 24
LANES = 128
SPLITS = 3
EARLY = 3

SIN_POLY = (4.442882919124345, -7.308245686509103, 3.6063542184332804, -0.8461116503752865, 0.10982451642699691)
COS_POLY = (1.4142134962552289, -6.978850948563853, 5.7394603769076955, -1.8835579059892091, 0.31068802753070307)


def horner(coefs, z):
    acc = jnp.float32(coefs[-1])
    for c in coefs[-2::-1]:
        acc = acc * z + jnp.float32(c)
    return acc


def cos_sin_turns(turns):
    r = turns - jnp.round(turns)
    z = r * r
    s = horner(SIN_POLY, z) * r
    c = horner(COS_POLY, z)
    return 1.0 - s * s, s * c


def split3(x):
    hi = x.astype(jnp.bfloat16)
    rest = x - hi.astype(jnp.float32)
    mid = rest.astype(jnp.bfloat16)
    lo = (rest - mid.astype(jnp.float32)).astype(jnp.bfloat16)
    return hi, mid, lo


def nt_dot(a, b):
    return lax.dot_general(a, b, (((1,), (1,)), ((), ())), preferred_element_type=jnp.float32)


def nn_dot(a, b):
    return jnp.dot(a, b, preferred_element_type=jnp.float32)


def pack_kernel(coef_ref, mil_ref, out_ref):
    half = coef_ref.shape[0] // 2
    ngroups = coef_ref.shape[1] // LANES
    m = mil_ref[...].astype(jnp.float32)
    mrows = [m[c : c + 1, g * LANES : (g + 1) * LANES] for c in range(3) for g in range(ngroups)]
    pad = out_ref.shape[2] - half * ngroups - len(mrows)
    if pad:
        mrows.append(jnp.zeros((pad, LANES), jnp.float32))
    mblock = jnp.concatenate(mrows, axis=0).astype(jnp.bfloat16)
    for h in range(2):
        rows = [
            coef_ref[h * half : (h + 1) * half, g * LANES : (g + 1) * LANES] for g in range(ngroups)
        ]
        block = jnp.concatenate(rows + [mblock], axis=0)
        for d in range(out_ref.shape[0]):
            out_ref[d, h] = block


def pack(coeffs_t, miller, ndev):
    nbl, npw = coeffs_t.shape
    ngroups = npw // LANES
    rows = -(-(nbl // 2 * ngroups + 3 * ngroups) // 8) * 8
    out = pl.pallas_call(
        pack_kernel,
        out_shape=jax.ShapeDtypeStruct((ndev // 2, 2, rows, LANES), jnp.bfloat16),
        name="pack",
    )(coeffs_t, miller)
    return out.reshape(ndev, rows, LANES)


def table_kernel(atc_ref, atr_ref, sp_ref, pos_ref, xc_ref, xr_ref, oc_ref, or_ref, *, kinds):
    natoms = sp_ref.shape[1]
    width = oc_ref.shape[2]
    per = width // SPLITS
    hi, mid, lo = split3(pos_ref[...])
    sp = sp_ref[...]
    row = lax.broadcasted_iota(jnp.int32, (width, natoms), 0) % per
    for at_ref, x_ref, o_ref in ((atc_ref, xc_ref, oc_ref), (atr_ref, xr_ref, or_ref)):
        n = at_ref.shape[0]
        pick = (lax.broadcasted_iota(jnp.int32, (n, natoms), 1) == at_ref[...]).astype(jnp.bfloat16)
        x = nt_dot(pick, hi) + nt_dot(pick, mid) + nt_dot(pick, lo)
        for c in range(3):
            x_ref[c] = jnp.broadcast_to(x[:, c : c + 1], (n, LANES))
        for s in range(SHELLS):
            kind_rows = ((row - s * kinds) == sp).astype(jnp.bfloat16)
            o_ref[s] = nt_dot(pick, kind_rows).astype(jnp.bfloat16)


def build(i, x_ref, o_ref, rads_ref, ms_ref, sel, put):
    n = x_ref.shape[1]
    ngroups = ms_ref.shape[2] // LANES
    step = 16 if n % 16 == 0 else n
    blocks = 4 if n % 64 == 0 else 1

    def select(s):
        sel[s, :n] = nn_dot(o_ref[s], rads_ref[i])

    def rows(first):
        m = [ms_ref[i, c : c + 1, :] for c in range(3)]
        for a in range(first, first + n // blocks, step):
            turns = 0.0
            for c in range(3):
                x = x_ref[c, a : a + step, :]
                turns = turns + jnp.concatenate([x] * ngroups, axis=1) * m[c]
            cos, sin = cos_sin_turns(turns)
            for s in range(SHELLS):
                v = sel[s, a : a + step, :]
                put(s * n + a, step, (v * cos).astype(jnp.bfloat16), (v * sin).astype(jnp.bfloat16))

    return [functools.partial(select, s) for s in range(SHELLS)] + [
        functools.partial(rows, k * (n // blocks)) for k in range(blocks)
    ]


def mingle(first, second):
    done = 0
    for k, piece in enumerate(first):
        piece()
        upto = (k + 1) * len(second) // len(first)
        for other in second[done:upto]:
            other()
        done = upto


def unrolled(count):
    return count <= 16


def early_kernel(
    ra_ref, xc_ref, xr_ref, oc_ref, or_ref, rad_ref,
    ms_ref, rads_ref, gca_ref, gsa_ref, gcc_ref, gsc_ref, sel_ref,
    *, nband, half, scale, qscale
):
    nga, _, npw = ms_ref.shape
    ngroups = npw // LANES
    qbins = rad_ref.shape[1]
    per = rads_ref.shape[1] // SPLITS
    first = half * ngroups

    def prepare(i):
        raw = ra_ref[i * nband, first:, :].astype(jnp.float32)
        comps = [
            jnp.concatenate([raw[c * ngroups + g : c * ngroups + g + 1] for g in range(ngroups)], axis=1)
            for c in range(3)
        ]
        for c in range(3):
            ms_ref[i, c : c + 1, :] = comps[c]
        q = (comps[0] * comps[0] + comps[1] * comps[1] + comps[2] * comps[2]) * jnp.float32(qscale)
        knot = lax.broadcasted_iota(jnp.int32, (qbins, npw), 0).astype(jnp.float32)
        hats = jnp.maximum(0.0, 1.0 - jnp.abs(q - knot))
        hi = hats.astype(jnp.bfloat16)
        lo = (hats - hi.astype(jnp.float32)).astype(jnp.bfloat16)
        table = rad_ref[...]
        r = nn_dot(table, hi) + nn_dot(table, lo)
        r = (r[0:per] + r[per : 2 * per] + r[2 * per : 3 * per]) * jnp.float32(scale)
        rads_ref[i] = jnp.concatenate(split3(r), axis=0)

    if unrolled(nga):
        for i in range(nga):
            prepare(i)
    else:
        def body(i, carry):
            prepare(i)
            return carry

        lax.fori_loop(0, nga, body, 0)

    def rebuild(i, slot):
        def put(row, count, c, s):
            gcc_ref[i, row : row + count, :] = c
            gsc_ref[i, row : row + count, :] = s

        return build(i, xr_ref, or_ref, rads_ref, ms_ref, sel_ref.at[slot], put)

    def start(i, slot):
        lanes = slice(i * npw, (i + 1) * npw)

        def put(row, count, c, s):
            gca_ref[row : row + count, lanes] = c
            gsa_ref[row : row + count, lanes] = s

        return build(i, xc_ref, oc_ref, rads_ref, ms_ref, sel_ref.at[slot], put)

    for i in range(gca_ref.shape[1] // npw):
        mingle(start(i, i % 2), [])
    for i in range(gcc_ref.shape[0]):
        mingle(rebuild(i, i % 2), [])


def main_kernel(
    ra_ref, rb_ref, xc_ref, xr_ref, oc_ref, or_ref, ms_ref, rads_ref, gc0_ref, gs0_ref,
    gce_ref, gse_ref, b_hbm,
    oth_ref, mine_ref, gcc_ref, gsc_ref,
    b_ref, sem, sel_ref, gca_ref, gsa_ref, cf_ref, acc_ref, proj_ref, mix_ref,
    *, nband, chunk, group,
):
    nga = ms_ref.shape[0]
    npw = ms_ref.shape[2]
    ngroups = npw // LANES
    half = oth_ref.shape[1] // nband
    nb = 2 * oth_ref.shape[1]
    nc = xc_ref.shape[1]
    nr = xr_ref.shape[1]
    nrows = b_ref.shape[0]
    early = gce_ref.shape[0] if unrolled(nga) else 0
    nsteps = nga // group

    copies = [
        pltpu.make_async_copy(b_hbm.at[pl.ds(k * chunk, chunk)], b_ref.at[pl.ds(k * chunk, chunk)], sem.at[k])
        for k in range(nrows // chunk)
    ]
    for copy in copies:
        copy.start()

    def weights(i):
        return [ms_ref[i, c : c + 1, :] * jnp.float32(1.0 / MMAX) for c in range(3)]

    def coefs(i):
        rows = []
        for ref in (ra_ref, rb_ref):
            for j in range(nband):
                rows.append(
                    jnp.concatenate(
                        [ref[i * nband + j, g * half : (g + 1) * half, :] for g in range(ngroups)], axis=1
                    )
                )
        return jnp.concatenate(rows, axis=0)

    def stage(step, slot, ready=False):
        pieces = []
        for e in range(group):
            i = step * group + e
            lanes = slice(e * npw, (e + 1) * npw)

            def put(row, count, c, s, lanes=lanes):
                gca_ref[slot, row : row + count, lanes] = c
                gsa_ref[slot, row : row + count, lanes] = s

            def scaled(i=i, lanes=lanes):
                c = coefs(i)
                cf = c.astype(jnp.float32)
                w = weights(i)
                cf_ref[slot, :nb, lanes] = c
                for k in range(3):
                    cf_ref[slot, (k + 1) * nb : (k + 2) * nb, lanes] = (cf * w[k]).astype(jnp.bfloat16)

            if not ready:
                pieces.extend(build(i, xc_ref, oc_ref, rads_ref, ms_ref, sel_ref.at[slot], put))
            pieces.append(scaled)
        return pieces

    def consume(gc, gs, slot):
        def cosines(s):
            rows = slice(s * nc, (s + 1) * nc)
            acc_ref[rows, :nb] += nt_dot(gc[rows, :], cf_ref[slot, :nb])

        def sines(s):
            rows = slice(s * nc, (s + 1) * nc)
            acc_ref[rows, nb:] += nt_dot(gs[rows, :], cf_ref[slot, nb:])

        return [functools.partial(f, s) for s in range(SHELLS) for f in (cosines, sines)]

    def consume_slot(slot):
        return consume(gca_ref.at[slot], gsa_ref.at[slot], slot)

    def clear(k, carry):
        acc_ref[pl.ds(pl.multiple_of(k * nc, 8), nc), :] = jnp.zeros((nc, acc_ref.shape[1]), jnp.float32)
        return carry

    lax.fori_loop(0, SHELLS, clear, 0)
    mingle(stage(0, 0, ready=True), [])
    last = consume(gc0_ref, gs0_ref, 0)
    if nsteps <= 8:
        for step in range(1, nsteps):
            mingle(stage(step, step % 2), last)
            last = consume_slot(step % 2)
    else:
        mingle(stage(1, 1), last)

        def body(step, carry):
            slot = step % 2
            mingle(stage(step, slot), consume_slot(1 - slot))
            return carry

        lax.fori_loop(2, nsteps, body, 0)
        last = consume_slot((nsteps - 1) % 2)
    mingle([lambda: None], last)

    for s in range(SHELLS):
        for t in range(COMPS):
            proj_ref[pl.ds(COMPS * s + t, nc, stride=NCH), :] = acc_ref[
                s * nc : (s + 1) * nc, t * nb : (t + 1) * nb
            ]
    proj = proj_ref[...].astype(jnp.bfloat16)

    def rebuild(i, slot):
        def put(row, count, c, s):
            gcc_ref[i - early, row : row + count, :] = c
            gsc_ref[i - early, row : row + count, :] = s

        return build(i, xr_ref, or_ref, rads_ref, ms_ref, sel_ref.at[slot], put)

    def multiply(first, count):
        mix_ref[first : first + count, :] = nn_dot(b_ref[first : first + count, :], proj)

    for copy in copies:
        copy.wait()
    nmul = nrows // chunk
    if unrolled(nga):
        for k in range(nmul):
            multiply(k * chunk, chunk)
            for i in range(early + k * (nga - early) // nmul, early + (k + 1) * (nga - early) // nmul):
                mingle(rebuild(i, i % 2), [])
    else:
        for k in range(nmul):
            multiply(k * chunk, chunk)

        def again(i, carry):
            mingle(rebuild(i, i % 2), [])
            return carry

        lax.fori_loop(0, nga, again, 0)

    mixed = []
    for t in range(COMPS):
        m = jnp.concatenate(
            [mix_ref[pl.ds(COMPS * s + t, nr, stride=NCH), :] for s in range(SHELLS)], axis=0
        )
        mixed.append(m.T)
    mine_ref[...] = jnp.concatenate([m[: nb // 2] for m in mixed], axis=0).astype(jnp.bfloat16)
    theirs = jnp.concatenate([m[nb // 2 :] for m in mixed], axis=0).astype(jnp.bfloat16)
    expand(theirs, ms_ref, gce_ref, gse_ref, gcc_ref, gsc_ref, oth_ref)


def expand(mixed, ms_ref, gce_ref, gse_ref, gcc_ref, gsc_ref, out_ref):
    nga = ms_ref.shape[0]
    rows = out_ref.shape[1]
    early = gce_ref.shape[0] if unrolled(nga) else 0

    def one(i):
        here = unrolled(nga) and i < early
        y = nn_dot(mixed[:rows], gce_ref[i] if here else gcc_ref[i - early])
        ys = nn_dot(mixed[rows:], gse_ref[i] if here else gsc_ref[i - early])
        for k in range(3):
            w = ms_ref[i, k : k + 1, :] * jnp.float32(1.0 / MMAX)
            y = y + w * ys[k * rows : (k + 1) * rows]
        out_ref[i] = y.astype(out_ref.dtype)

    if unrolled(nga):
        for i in range(nga):
            one(i)
    else:
        def body(i, carry):
            one(i)
            return carry

        lax.fori_loop(0, nga, body, 0)


def own_kernel(mine_ref, ms_ref, gce_ref, gse_ref, gcc_ref, gsc_ref, own_ref):
    expand(mine_ref[...], ms_ref, gce_ref, gse_ref, gcc_ref, gsc_ref, own_ref)


def row_chunk(count):
    for cand in range(min(count, 256), 0, -1):
        if count % cand == 0 and cand % 8 == 0:
            return cand
    return count


def finish_kernel(recv_ref, coef_ref, out_ref):
    n = recv_ref.shape[0]
    parts = []
    for h in range(2):
        def add(k, acc, h=h):
            return acc + recv_ref[k, h].astype(jnp.float32)
        parts.append(lax.fori_loop(0, n, add, jnp.zeros(recv_ref.shape[2:], jnp.float32), unroll=8))
    total = jnp.concatenate(parts, axis=0)
    out_ref[...] = (coef_ref[...].astype(jnp.float32) + total).astype(out_ref.dtype)


def shards(coeffs, coupling, miller, species, proj_atom, positions, radial):
    nga = lax.axis_size("ga")
    nband = lax.axis_size("band")
    ndev = nga * nband
    axes = ("ga", "band")
    npw, nbl = coeffs.shape
    half = nbl // 2
    nb = nbl * nband
    nrows, ncols = coupling.shape
    nr, nc = nrows // NCH, ncols // NCH
    kinds = radial.shape[0] // SHELLS
    qbins = radial.shape[1]
    natoms = species.shape[0]
    scale = 1.0 / math.sqrt(npw * nga)
    pair = [(k, k ^ 1) for k in range(nband)]

    coeffs_t = coeffs.T
    sent = pack(coeffs_t, miller, ndev)
    ra = lax.all_to_all(sent, axes, 0, 0)
    i = lax.axis_index("ga")
    j = lax.axis_index("band")
    atoms_c = lax.dynamic_slice_in_dim(proj_atom, j * ncols, ncols).reshape(nc, NCH)[:, :1]
    atoms_r = lax.dynamic_slice_in_dim(proj_atom, i * nrows, nrows).reshape(nr, NCH)[:, :1]
    per = -(-SHELLS * kinds // 16) * 16
    table = radial.reshape(kinds, SHELLS, qbins).transpose(1, 0, 2).reshape(SHELLS * kinds, qbins)
    table = jnp.pad(table, ((0, per - SHELLS * kinds), (0, 0)))
    hi = lax.reduce_precision(table, 8, 7)
    mid = lax.reduce_precision(table - hi, 8, 7)
    lo = table - hi - mid
    table = jnp.concatenate([hi, mid, lo], axis=0).astype(jnp.bfloat16)
    width = SPLITS * per
    xc, xr, oc, orr = pl.pallas_call(
        functools.partial(table_kernel, kinds=kinds),
        out_shape=[
            jax.ShapeDtypeStruct((3, nc, LANES), jnp.float32),
            jax.ShapeDtypeStruct((3, nr, LANES), jnp.float32),
            jax.ShapeDtypeStruct((SHELLS, nc, width), jnp.bfloat16),
            jax.ShapeDtypeStruct((SHELLS, nr, width), jnp.bfloat16),
        ],
        cost_estimate=pl.CostEstimate(flops=10**9, transcendentals=0, bytes_accessed=10**6),
        compiler_params=pltpu.CompilerParams(vmem_limit_bytes=16 * 1024 * 1024),
        name="tables",
    )(atoms_c, atoms_r, species.reshape(1, natoms), positions)

    ra, table, xc, xr, oc, orr = lax.optimization_barrier((ra, table, xc, xr, oc, orr))
    rb = lax.ppermute(ra, "band", pair)

    chunk = row_chunk(nrows)
    vmem = pl.BlockSpec(memory_space=pltpu.VMEM)
    nmax = max(nc, nr)
    group = 2 if nga % 2 == 0 else 1
    early = min(EARLY, nga // 2)
    kept = nga - early if unrolled(nga) else nga
    ms, rads, gc0, gs0, gce, gse = pl.pallas_call(
        functools.partial(
            early_kernel, nband=nband, half=half, scale=scale, qscale=(qbins - 1) / (3.0 * MMAX * MMAX)
        ),
        out_shape=[
            jax.ShapeDtypeStruct((nga, 8, npw), jnp.float32),
            jax.ShapeDtypeStruct((nga, width, npw), jnp.bfloat16),
            jax.ShapeDtypeStruct((SHELLS * nc, group * npw), jnp.bfloat16),
            jax.ShapeDtypeStruct((SHELLS * nc, group * npw), jnp.bfloat16),
            jax.ShapeDtypeStruct((early, SHELLS * nr, npw), jnp.bfloat16),
            jax.ShapeDtypeStruct((early, SHELLS * nr, npw), jnp.bfloat16),
        ],
        scratch_shapes=[pltpu.VMEM((2, SHELLS, nmax, npw), jnp.float32)],
        compiler_params=pltpu.CompilerParams(vmem_limit_bytes=32 * 1024 * 1024),
        cost_estimate=pl.CostEstimate(flops=10**9, transcendentals=0, bytes_accessed=10**6),
        name="early",
    )(ra, xc, xr, oc, orr, table)
    other, mine, gcc, gsc = pl.pallas_call(
        functools.partial(main_kernel, nband=nband, chunk=chunk, group=group),
        in_specs=[vmem] * 12 + [pl.BlockSpec(memory_space=pl.ANY)],
        out_specs=[vmem] * 4,
        out_shape=[
            jax.ShapeDtypeStruct((nga, nb // 2, npw), jnp.bfloat16),
            jax.ShapeDtypeStruct((COMPS * nb // 2, SHELLS * nr), jnp.bfloat16),
            jax.ShapeDtypeStruct((kept, SHELLS * nr, npw), jnp.bfloat16),
            jax.ShapeDtypeStruct((kept, SHELLS * nr, npw), jnp.bfloat16),
        ],
        scratch_shapes=[
            pltpu.VMEM((nrows, ncols), jnp.bfloat16),
            pltpu.SemaphoreType.DMA((nrows // chunk,)),
            pltpu.VMEM((2, SHELLS, nmax, npw), jnp.float32),
            pltpu.VMEM((2, SHELLS * nc, group * npw), jnp.bfloat16),
            pltpu.VMEM((2, SHELLS * nc, group * npw), jnp.bfloat16),
            pltpu.VMEM((2, COMPS * nb, group * npw), jnp.bfloat16),
            pltpu.VMEM((SHELLS * nc, COMPS * nb), jnp.float32),
            pltpu.VMEM((ncols, nb), jnp.float32),
            pltpu.VMEM((nrows, nb), jnp.float32),
        ],
        compiler_params=pltpu.CompilerParams(vmem_limit_bytes=46 * 1024 * 1024),
        name="apply",
    )(ra, rb, xc, xr, oc, orr, ms, rads, gc0, gs0, gce, gse, coupling)

    theirs = lax.ppermute(other, "band", pair)
    own = pl.pallas_call(
        own_kernel,
        out_shape=jax.ShapeDtypeStruct((nga, nb // 2, npw), jnp.float32),
        compiler_params=pltpu.CompilerParams(vmem_limit_bytes=32 * 1024 * 1024),
        cost_estimate=pl.CostEstimate(flops=10**9, transcendentals=0, bytes_accessed=10**6),
        name="own",
    )(mine, ms, gce, gse, gcc, gsc)
    pairs = (own + theirs.astype(jnp.float32)).astype(jnp.bfloat16).reshape(ndev, half, npw)
    back = lax.all_to_all(pairs, axes, 0, 0).reshape(ndev // 2, 2, half, npw)
    return pl.pallas_call(
        finish_kernel,
        out_shape=jax.ShapeDtypeStruct((nbl, npw), jnp.bfloat16),
        compiler_params=pltpu.CompilerParams(vmem_limit_bytes=16 * 1024 * 1024),
        name="finish",
    )(back, coeffs_t).T


def solution(mesh):
    placed = (P("ga", "band"), P("ga", "band"), P(None, "ga"), P(), P(), P(), P())
    return jax.shard_map(
        shards, mesh=mesh, in_specs=placed, out_specs=P("ga", "band"), check_vma=False
    )
```
